16 devices in a mesh: dp: 4 (over z, y), fsdp: 4 (over x, core).
Axes of the slice: x: 2, y: 2, z: 2, core: 2. Of those that a mesh axis runs over, the one named last changes fastest.
Arguments:
- x_in: bfloat16 [64, 512, 768], P(('dp', 'fsdp'))
- grad_y: bfloat16 [64, 512, 768], P(('dp', 'fsdp'))
- norm_scale: bfloat16 [2, 768], P(None, 'fsdp')
- w_in: bfloat16 [2, 768, 7040], P(None, 'fsdp')
- w_out: bfloat16 [2, 3840, 768], P(None, 'fsdp')
Outputs:
- output 1: bfloat16 [64, 512, 768], P(('dp', 'fsdp'))
- output 2: bfloat16 [64, 512, 768], P(('dp', 'fsdp'))
- output 3: float32 [2, 768], P(None, 'fsdp')
- output 4: float32 [2, 768, 7040], P(None, 'fsdp')
- output 5: float32 [2, 3840, 768], P(None, 'fsdp')
All inputs are finite; a program needn't handle non-finite values.
Results may differ from the reference program's by a relative error of at most 0.0162002.
Values are sent between devices in bfloat16 or wider.
A program may use at most 1 GiB of HBM per device.

```python
import jax
import jax.numpy as jnp
from jax import lax

MODEL_DIM = 768
N_HEADS = 12
HEAD_DIM = 64
FF_DIM = 3072
SEQ_LEN = 512
BATCH = 64
N_LAYERS = 2

PROJ_DIM = MODEL_DIM + 2 * HEAD_DIM + 2 * FF_DIM
CAT_DIM = MODEL_DIM + FF_DIM


def setup_inputs(seed: int = 0) -> dict:
    rng_keys = jax.random.split(jax.random.key(seed), 5)
    x_in = jax.random.normal(rng_keys[0], (BATCH, SEQ_LEN, MODEL_DIM), jnp.float32)
    grad_y = jax.random.normal(rng_keys[1], (BATCH, SEQ_LEN, MODEL_DIM), jnp.float32)
    norm_scale = 1.0 + 0.3 * jax.random.normal(rng_keys[2], (N_LAYERS, MODEL_DIM), jnp.float32)
    w_in = jax.random.normal(rng_keys[3], (N_LAYERS, MODEL_DIM, PROJ_DIM), jnp.float32) * MODEL_DIM ** -0.5
    w_out = jax.random.normal(rng_keys[4], (N_LAYERS, CAT_DIM, MODEL_DIM), jnp.float32) * CAT_DIM ** -0.5
    return {
        "x_in": x_in.astype(jnp.bfloat16),
        "grad_y": grad_y.astype(jnp.bfloat16),
        "norm_scale": norm_scale.astype(jnp.bfloat16),
        "w_in": w_in.astype(jnp.bfloat16),
        "w_out": w_out.astype(jnp.bfloat16),
    }


def layer_norm(hidden, gain_vec):
    hid_f32 = hidden.astype(jnp.float32)
    centered = hid_f32 - jnp.mean(hid_f32, axis=-1, keepdims=True)
    variance = jnp.mean(centered * centered, axis=-1, keepdims=True)
    return (centered * lax.rsqrt(variance + 1e-6) * gain_vec).astype(jnp.bfloat16)


def rotary_tables():
    half_dim = HEAD_DIM // 2
    inv_freq = 10000.0 ** (-(jnp.arange(half_dim, dtype=jnp.float32) * 2.0 / HEAD_DIM))
    angles = jnp.arange(SEQ_LEN, dtype=jnp.float32)[:, None] * inv_freq[None, :]
    return jnp.cos(angles), jnp.sin(angles)


def rotate(vectors, cos_tab, sin_tab):
    half_dim = vectors.shape[-1] // 2
    lo_half = vectors[..., :half_dim]
    hi_half = vectors[..., half_dim:]
    return jnp.concatenate([lo_half * cos_tab - hi_half * sin_tab, hi_half * cos_tab + lo_half * sin_tab], axis=-1)


def mix_seq(projected):
    kv_end = MODEL_DIM + 2 * HEAD_DIM
    queries = projected[:, :MODEL_DIM].reshape(SEQ_LEN, N_HEADS, HEAD_DIM).astype(jnp.float32) * HEAD_DIM ** -0.5
    key_vec = projected[:, MODEL_DIM:MODEL_DIM + HEAD_DIM].astype(jnp.float32)
    val_vec = projected[:, MODEL_DIM + HEAD_DIM:kv_end].astype(jnp.float32)
    gate_act = projected[:, kv_end:kv_end + FF_DIM].astype(jnp.float32)
    up_act = projected[:, kv_end + FF_DIM:].astype(jnp.float32)
    cos_tab, sin_tab = rotary_tables()
    q_rot = rotate(queries, cos_tab[:, None, :], sin_tab[:, None, :]).astype(jnp.bfloat16).astype(jnp.float32)
    k_rot = rotate(key_vec, cos_tab, sin_tab).astype(jnp.bfloat16).astype(jnp.float32)
    scores = jnp.einsum("qhd,kd->hqk", q_rot, k_rot)
    positions = jnp.arange(SEQ_LEN)
    scores = jnp.where(positions[:, None] >= positions[None, :], scores, -1e30)
    attn_probs = jax.nn.softmax(scores, axis=-1).astype(jnp.bfloat16).astype(jnp.float32)
    attn_out = jnp.einsum("hqk,kd->qhd", attn_probs, val_vec).astype(jnp.bfloat16).reshape(SEQ_LEN, MODEL_DIM)
    mlp_out = (jax.nn.silu(gate_act) * up_act).astype(jnp.bfloat16)
    return jnp.concatenate([attn_out, mlp_out], axis=-1)


def mix_backward(seq_pair):
    projected, grad_mixed = seq_pair
    return jax.vjp(mix_seq, projected)[1](grad_mixed)[0]


def layer_forward(hidden, gain_vec, w_in_l, w_out_l):
    normed = layer_norm(hidden, gain_vec.astype(jnp.float32))
    projected = jnp.dot(normed.reshape(-1, MODEL_DIM), w_in_l, preferred_element_type=jnp.float32).astype(jnp.bfloat16)
    projected = projected.reshape(BATCH, SEQ_LEN, PROJ_DIM)
    mixed_out = lax.map(mix_seq, projected)
    block_out = jnp.dot(mixed_out.reshape(-1, CAT_DIM), w_out_l, preferred_element_type=jnp.float32)
    layer_out = (hidden.astype(jnp.float32) + block_out.reshape(BATCH, SEQ_LEN, MODEL_DIM)).astype(jnp.bfloat16)
    return layer_out, normed, projected, mixed_out


def layer_backward(hidden, gain_vec, w_in_l, w_out_l, grad_out):
    normed, projected, mixed_out = layer_forward(hidden, gain_vec, w_in_l, w_out_l)[1:]
    grad_rows = grad_out.reshape(-1, MODEL_DIM)
    grad_w_out = jnp.dot(mixed_out.reshape(-1, CAT_DIM).T, grad_rows, preferred_element_type=jnp.float32)
    grad_mixed = jnp.dot(grad_rows, w_out_l.T, preferred_element_type=jnp.float32).astype(jnp.bfloat16)
    grad_proj = lax.map(mix_backward, (projected, grad_mixed.reshape(BATCH, SEQ_LEN, CAT_DIM)))
    grad_proj_rows = grad_proj.reshape(-1, PROJ_DIM)
    grad_w_in = jnp.dot(normed.reshape(-1, MODEL_DIM).T, grad_proj_rows, preferred_element_type=jnp.float32)
    grad_normed = jnp.dot(grad_proj_rows, w_in_l.T, preferred_element_type=jnp.float32).astype(jnp.bfloat16)
    norm_vjp = jax.vjp(layer_norm, hidden, gain_vec.astype(jnp.float32))[1]
    grad_hidden, grad_gain = norm_vjp(grad_normed.reshape(BATCH, SEQ_LEN, MODEL_DIM))
    grad_in = (grad_out.astype(jnp.float32) + grad_hidden.astype(jnp.float32)).astype(jnp.bfloat16)
    return grad_in, grad_gain, grad_w_in, grad_w_out


def reference(x_in, grad_y, norm_scale, w_in, w_out):
    layer_inputs = []
    hidden = x_in
    for layer_idx in range(N_LAYERS):
        layer_inputs.append(hidden)
        hidden = layer_forward(hidden, norm_scale[layer_idx], w_in[layer_idx], w_out[layer_idx])[0]
    grad_hidden = grad_y
    scale_grads = []
    in_grads = []
    out_grads = []
    for layer_idx in reversed(range(N_LAYERS)):
        grad_hidden, grad_gain, grad_w_in, grad_w_out = layer_backward(
            layer_inputs[layer_idx], norm_scale[layer_idx], w_in[layer_idx], w_out[layer_idx], grad_hidden)
        scale_grads.append(grad_gain)
        in_grads.append(grad_w_in)
        out_grads.append(grad_w_out)
    return (hidden, grad_hidden, jnp.stack(scale_grads[::-1]), jnp.stack(in_grads[::-1]), jnp.stack(out_grads[::-1]))
```

```python
import functools
import jax
import jax.numpy as jnp
import numpy as np
from jax import lax
from jax.experimental import pallas as pl
from jax.experimental.pallas import tpu as pltpu
from jax.sharding import PartitionSpec as P

F32 = jnp.float32
BF16 = jnp.bfloat16
VMEM_LIMIT = 67_043_328


def dot_nn(lhs, rhs):
    return lax.dot_general(lhs, rhs, (((1,), (0,)), ((), ())), preferred_element_type=F32)


def dot_nt(lhs, rhs):
    return lax.dot_general(lhs, rhs, (((1,), (1,)), ((), ())), preferred_element_type=F32)


def dot_tn(lhs, rhs):
    return lax.dot_general(lhs, rhs, (((0,), (0,)), ((), ())), preferred_element_type=F32)


def rotary_tables(seq_len, head_dim):
    half_dim = head_dim // 2
    inv_freq = 10000.0 ** (-(np.arange(half_dim, dtype=np.float64) * 2.0 / head_dim))
    angles = np.arange(seq_len, dtype=np.float64)[:, None] * inv_freq[None, :]
    cos_tab = np.tile(np.cos(angles), (1, 128 // half_dim))
    sin_tab = np.tile(np.concatenate([-np.sin(angles), np.sin(angles)], axis=1), (1, 128 // head_dim))
    return cos_tab.astype(np.float32), sin_tab.astype(np.float32)


def swap_halves(block):
    lane = lax.broadcasted_iota(jnp.int32, block.shape, 1)
    return jnp.where((lane & 63) < 32, pltpu.roll(block, 96, 1), pltpu.roll(block, 32, 1))


def lower_lanes(shape):
    return lax.broadcasted_iota(jnp.int32, shape, 1) < 64


def normalize(hidden):
    centered = hidden - jnp.mean(hidden, axis=-1, keepdims=True)
    variance = jnp.mean(centered * centered, axis=-1, keepdims=True)
    rstd = lax.rsqrt(variance + 1e-6)
    return centered * rstd, rstd


def forward_kernel(x_ref, g_ref, win_ref, cos_ref, sin_ref, h_ref, z_ref, gu_ref, om_ref, k_lo, k_hi, v_lo, v_hi, *, dims):
    model_dim, ff_dim, seq_len, chunk, q_block = dims
    kv_end = model_dim + 128
    x = x_ref[0].astype(F32)
    h = (normalize(x)[0] * g_ref[...]).astype(BF16)
    h_ref[0] = h
    z_ref[0] = dot_nn(h, win_ref[:, :kv_end]).astype(BF16)

    kv = z_ref[0, :, model_dim:kv_end].astype(F32)
    low = lower_lanes(kv.shape)
    k_rot = jnp.where(low, kv * cos_ref[...] + swap_halves(kv) * sin_ref[...], 0.0)
    k_lo[...] = k_rot.astype(BF16)
    k_hi[...] = pltpu.roll(k_rot, 64, 1).astype(BF16)
    val = jnp.where(low, 0.0, kv)
    v_hi[...] = val.astype(BF16)
    v_lo[...] = pltpu.roll(val, 64, 1).astype(BF16)

    def head_pair(pair, carry):
        cols = pl.ds(pl.multiple_of(pair * 128, 128), 128)
        q = z_ref[0, :, cols].astype(F32) * 0.125
        q = (q * cos_ref[...] + swap_halves(q) * sin_ref[...]).astype(BF16)
        for blk in range(seq_len // q_block):
            start, n_keys = blk * q_block, (blk + 1) * q_block
            q_blk = q[start:n_keys]
            row = lax.broadcasted_iota(jnp.int32, (q_block, n_keys), 0) + start
            causal = row >= lax.broadcasted_iota(jnp.int32, (q_block, n_keys), 1)
            out = None
            for k_ref, v_ref in ((k_lo, v_lo), (k_hi, v_hi)):
                scores = jnp.where(causal, dot_nt(q_blk, k_ref[:n_keys]), -1e30)
                probs = jnp.exp(scores - jnp.max(scores, axis=-1, keepdims=True))
                probs = probs * (1.0 / jnp.sum(probs, axis=-1, keepdims=True))
                part = dot_nn(probs.astype(BF16), v_ref[:n_keys])
                out = part if out is None else out + part
            om_ref[0, start:n_keys, cols] = out.astype(BF16)
        return carry

    lax.fori_loop(0, model_dim // 128, head_pair, 0)

    def ff_chunk(idx, carry):
        base = pl.multiple_of(idx * chunk, 128)
        gate_cols = pl.ds(base, chunk)
        up_cols = pl.ds(pl.multiple_of(ff_dim + base, 128), chunk)
        gate = dot_nn(h_ref[0], win_ref[:, pl.ds(pl.multiple_of(kv_end + base, 128), chunk)]).astype(BF16)
        up = dot_nn(h_ref[0], win_ref[:, pl.ds(pl.multiple_of(kv_end + ff_dim + base, 128), chunk)]).astype(BF16)
        gu_ref[0, :, gate_cols] = gate
        gu_ref[0, :, up_cols] = up
        gate = gate.astype(F32)
        mid = gate * jax.nn.sigmoid(gate) * up.astype(F32)
        om_ref[0, :, pl.ds(pl.multiple_of(model_dim + base, 128), chunk)] = mid.astype(BF16)
        return carry

    lax.fori_loop(0, ff_dim // chunk, ff_chunk, 0)


def mlp_backward_kernel(dy_ref, gu_ref, wout_ref, dgu_ref, *, dims):
    model_dim, ff_dim, seq_len, chunk, q_block = dims

    def ff_chunk(idx, carry):
        base = pl.multiple_of(idx * chunk, 128)
        gate_cols = pl.ds(base, chunk)
        up_cols = pl.ds(pl.multiple_of(ff_dim + base, 128), chunk)
        d_mid = dot_nt(dy_ref[0], wout_ref[pl.ds(pl.multiple_of(model_dim + base, 128), chunk), :]).astype(BF16).astype(F32)
        gate = gu_ref[0, :, gate_cols].astype(F32)
        up = gu_ref[0, :, up_cols].astype(F32)
        sig = jax.nn.sigmoid(gate)
        act = gate * sig
        dgu_ref[0, :, up_cols] = (d_mid * act).astype(BF16)
        dgu_ref[0, :, gate_cols] = (d_mid * up * (sig + act * (1.0 - sig))).astype(BF16)
        return carry

    lax.fori_loop(0, ff_dim // chunk, ff_chunk, 0)


def attention_backward_kernel(dy_ref, z_ref, wout_ref, cos_ref, sin_ref, dz_ref,
                              do_ref, k_lo, k_hi, k_dup, v_dup, dk_acc, dv_acc, *, dims):
    model_dim, ff_dim, seq_len, chunk, q_block = dims
    kv_end = model_dim + 128
    do_ref[...] = dot_nt(dy_ref[0], wout_ref[:model_dim, :]).astype(BF16)
    kv = z_ref[0, :, model_dim:kv_end].astype(F32)
    low = lower_lanes(kv.shape)
    k_rot = jnp.where(low, kv * cos_ref[...] + swap_halves(kv) * sin_ref[...], 0.0)
    k_up = pltpu.roll(k_rot, 64, 1)
    k_lo[...] = k_rot.astype(BF16)
    k_hi[...] = k_up.astype(BF16)
    k_dup[...] = (k_rot + k_up).astype(BF16)
    v_dup[...] = jnp.where(low, pltpu.roll(kv, 64, 1), kv).astype(BF16)
    dk_acc[...] = jnp.zeros_like(dk_acc)
    dv_acc[...] = jnp.zeros_like(dv_acc)

    def head_pair(pair, carry):
        cols = pl.ds(pl.multiple_of(pair * 128, 128), 128)
        q = z_ref[0, :, cols].astype(F32) * 0.125
        q = q * cos_ref[...] + swap_halves(q) * sin_ref[...]
        d_out = do_ref[:, cols].astype(F32)
        for blk in range(seq_len // q_block):
            start, n_keys = blk * q_block, (blk + 1) * q_block
            low_q = lower_lanes((q_block, 128))
            q_blk = q[start:n_keys]
            do_blk = d_out[start:n_keys]
            q_two = jnp.concatenate([jnp.where(low_q, q_blk, 0.0), jnp.where(low_q, 0.0, q_blk)], axis=0).astype(BF16)
            do_two = jnp.concatenate([jnp.where(low_q, do_blk, 0.0), jnp.where(low_q, 0.0, do_blk)], axis=0).astype(BF16)
            shape = (n_keys, 2 * q_block)
            query = (lax.broadcasted_iota(jnp.int32, shape, 1) & (q_block - 1)) + start
            causal = query >= lax.broadcasted_iota(jnp.int32, shape, 0)
            scores = jnp.where(causal, dot_nt(k_dup[:n_keys], q_two), -1e30)
            probs = jnp.exp(scores - jnp.max(scores, axis=0, keepdims=True))
            probs = probs * (1.0 / jnp.sum(probs, axis=0, keepdims=True))
            d_probs = dot_nt(v_dup[:n_keys], do_two).astype(BF16).astype(F32)
            d_scores = (probs * (d_probs - jnp.sum(probs * d_probs, axis=0, keepdims=True))).astype(BF16)
            dv_acc[:n_keys] += dot_nn(probs.astype(BF16), do_two)
            dk_acc[:n_keys] += dot_nn(d_scores, q_two)
            dq = dot_tn(d_scores[:, :q_block], k_lo[:n_keys]) + dot_tn(d_scores[:, q_block:], k_hi[:n_keys])
            dq = dq.astype(BF16).astype(F32)
            dq = dq * cos_ref[start:n_keys] - swap_halves(dq) * sin_ref[start:n_keys]
            dz_ref[0, start:n_keys, cols] = (dq * 0.125).astype(BF16)
        return carry

    lax.fori_loop(0, model_dim // 128, head_pair, 0)
    dk = dk_acc[...]
    dk = (dk + pltpu.roll(dk, 64, 1)).astype(BF16).astype(F32)
    dk = dk * cos_ref[...] - swap_halves(dk) * sin_ref[...]
    dv = dv_acc[...]
    dv = dv + pltpu.roll(dv, 64, 1)
    dz_ref[0, :, model_dim:kv_end] = jnp.where(low, dk, dv).astype(BF16)


def input_backward_kernel(dy_ref, x_ref, g_ref, dz_ref, dgu_ref, win_ref, dx_ref, dg_ref, dh_ref, *, dims):
    model_dim = dims[0]
    kv_end = model_dim + 128
    for start in range(0, model_dim, 256):
        rows = slice(start, start + 256)
        dh = dot_nt(dgu_ref[0], win_ref[rows, kv_end:]) + dot_nt(dz_ref[0], win_ref[rows, :kv_end])
        dh_ref[:, rows] = dh.astype(BF16)
    x_hat, rstd = normalize(x_ref[0].astype(F32))
    dh = dh_ref[...].astype(F32)
    d_gain = jnp.sum(dh * x_hat, axis=0, keepdims=True)

    @pl.when(pl.program_id(0) == 0)
    def _():
        dg_ref[...] = d_gain

    @pl.when(pl.program_id(0) > 0)
    def _():
        dg_ref[...] += d_gain

    d_hat = dh * g_ref[...]
    d_in = rstd * (d_hat - jnp.mean(d_hat, axis=-1, keepdims=True)
                   - x_hat * jnp.mean(d_hat * x_hat, axis=-1, keepdims=True))
    dx_ref[0] = (dy_ref[0].astype(F32) + d_in.astype(BF16).astype(F32)).astype(BF16)


def seq_spec(seq_len, width):
    return pl.BlockSpec((1, seq_len, width), lambda i: (i, 0, 0))


WHOLE = pl.BlockSpec(memory_space=pltpu.VMEM)


def seq_call(kernel, name, n_seq, seq_inputs, whole_inputs, order, seq_outputs, whole_outputs, scratch, flops, seq_len):
    specs = {True: lambda a: seq_spec(seq_len, a.shape[2]), False: lambda a: WHOLE}
    inputs = [(seq_inputs if kind else whole_inputs).pop(0) for kind in order]
    shapes = [jax.ShapeDtypeStruct((n_seq, seq_len, w), BF16) for w in seq_outputs]
    shapes += [jax.ShapeDtypeStruct(w, F32) for w in whole_outputs]
    out_specs = [seq_spec(seq_len, w) for w in seq_outputs] + [pl.BlockSpec(w, lambda i: (0, 0)) for w in whole_outputs]
    return pl.pallas_call(
        kernel,
        grid=(n_seq,),
        out_shape=shapes,
        in_specs=[specs[kind](a) for kind, a in zip(order, inputs)],
        out_specs=out_specs,
        scratch_shapes=scratch,
        compiler_params=pltpu.CompilerParams(dimension_semantics=("arbitrary",), vmem_limit_bytes=VMEM_LIMIT),
        cost_estimate=pl.CostEstimate(flops=flops, bytes_accessed=50_000_000, transcendentals=0),
        name=name,
    )(*inputs)


def layer_forward(x, gain, w_in, tables, dims):
    model_dim, ff_dim, seq_len = dims[:3]
    return seq_call(functools.partial(forward_kernel, dims=dims), "layer_forward", x.shape[0],
                    [x], [gain, w_in, *tables], (True, False, False, False, False),
                    [model_dim, model_dim + 128, 2 * ff_dim, model_dim + ff_dim], [],
                    [pltpu.VMEM((seq_len, 128), BF16)] * 4,
                    2 * x.shape[0] * seq_len * model_dim * (w_in.shape[1] + 4 * seq_len), seq_len)


def mlp_backward(dy, gu, w_out, dims):
    model_dim, ff_dim, seq_len = dims[:3]
    return seq_call(functools.partial(mlp_backward_kernel, dims=dims), "mlp_backward", dy.shape[0],
                    [dy, gu], [w_out], (True, True, False), [2 * ff_dim], [], [],
                    2 * dy.shape[0] * seq_len * model_dim * ff_dim, seq_len)[0]


def attention_backward(dy, z, w_out, tables, dims):
    model_dim, ff_dim, seq_len = dims[:3]
    small = pltpu.VMEM((seq_len, 128), BF16)
    wide = pltpu.VMEM((seq_len, 128), F32)
    return seq_call(functools.partial(attention_backward_kernel, dims=dims), "attention_backward", dy.shape[0],
                    [dy, z], [w_out, *tables], (True, True, False, False, False), [model_dim + 128], [],
                    [pltpu.VMEM((seq_len, model_dim), BF16), small, small, small, small, wide, wide],
                    2 * dy.shape[0] * seq_len * model_dim * (model_dim + 10 * seq_len), seq_len)[0]


def input_backward(dy, x, gain, dz, dgu, w_in, dims):
    model_dim, ff_dim, seq_len = dims[:3]
    return seq_call(functools.partial(input_backward_kernel, dims=dims), "input_backward", dy.shape[0],
                    [dy, x, dz, dgu], [gain, w_in], (True, True, False, True, True, False), [model_dim], [(1, model_dim)],
                    [pltpu.VMEM((seq_len, model_dim), BF16)],
                    2 * dy.shape[0] * seq_len * model_dim * w_in.shape[1], seq_len)


LINKS = {"core": ("fsdp", 1), "x": ("fsdp", 2), "y": ("dp", 1), "z": ("dp", 2)}


def swap(value, link):
    axis, bit = LINKS[link]
    return lax.ppermute(value, axis, [(i, i ^ bit) for i in range(4)])


def my_bit(link):
    axis, bit = LINKS[link]
    return (lax.axis_index(axis) // bit) % 2


def pick(value, index, dim):
    return lax.dynamic_index_in_dim(value, index, dim, keepdims=False)


ORDERS = (("x", "y", "z"), ("y", "z", "x"), ("z", "x", "y"))
DIMS = ("x", "core", "y", "z")


class Reduction:
    def __init__(self, part, sent=None, relay="y"):
        core = my_bit("core")
        self.stage, self.relay = 0, relay
        self.cols = (part if sent is None else sent).shape[1]
        if sent is None:
            self.part = self.view(part, 2)
            self.sent = self.cut(self.part, {"core": 1 - core})
        else:
            self.part, self.sent = part, self.view(sent, 1)
        self.picks = [{"core": core} for _ in range(3)]
        self.terms = [[], [], []]

    def view(self, value, cores):
        rows = value.shape[0] // (2 * cores * 12)
        return value.reshape(2, cores, 2, 2, 3, rows, self.cols)

    def cut(self, term, picks, third=None):
        starts, sizes = [], []
        for dim, size in zip(DIMS, term.shape):
            starts.append(picks[dim] if dim in picks and size == 2 else 0)
            sizes.append(1 if dim in picks else size)
        whole = third is None or term.shape[4] == 1
        starts += [0 if whole else third, 0, 0]
        sizes += [term.shape[4] if whole else 1, *term.shape[5:]]
        return lax.dynamic_slice(term, starts, sizes)

    def total(self, third, picks):
        return sum(self.cut(t, picks, third) for t in self.terms[third])

    def prepare(self):
        if self.stage == 0:
            return [self.sent]
        if self.stage == 1:
            part = self.part if self.part.ndim == 7 else self.view(self.part, 1)
            self.terms = [[part, self.received[0]] for _ in range(3)]
        elif self.stage <= 4:
            for terms, received in zip(self.terms, self.received):
                terms.append(received)
        if self.stage <= 3:
            sends = []
            for third, order in enumerate(ORDERS):
                link = order[self.stage - 1]
                bit = my_bit(link)
                sends.append(self.total(third, {**self.picks[third], link: 1 - bit}))
                self.picks[third][link] = bit
            return sends
        if self.stage == 4:
            return [jnp.concatenate([self.total(third, self.picks[third]) for third in range(3)], axis=4)]
        return [self.received[0 if self.relay == "z" else 1]]

    def launch(self, sends):
        if self.stage == 0:
            self.received = [swap(sends[0], "core")]
        elif self.stage <= 3:
            self.received = [swap(s, order[self.stage - 1]) for s, order in zip(sends, ORDERS)]
        elif self.stage == 4:
            self.own = sends[0]
            self.received = [swap(self.own, "y"), swap(self.own, "z")]
        else:
            self.last = swap(sends[0], self.relay)
        self.stage += 1

    def place(self, out, layer_idx, col, start=0, width=None):
        for piece, flip_y, flip_z in ((self.own, 0, 0), (self.received[0], 1, 0), (self.received[1], 0, 1), (self.last, 1, 1)):
            block = piece.reshape(1, -1, self.cols)[:, :, start:start + (width or self.cols)]
            row = (((my_bit("y") + flip_y) % 2) * 2 + (my_bit("z") + flip_z) % 2) * block.shape[1]
            out = lax.dynamic_update_slice(out, block, (layer_idx, row, col))
        return out


class SmallSum:
    def __init__(self, value):
        self.value, self.links = value, ["core", "x", "y", "z"]

    def prepare(self):
        return [self.value]

    def launch(self, sends):
        self.value = sends[0] + swap(sends[0], self.links.pop(0))


def advance(reductions, *inputs):
    sends, inputs = lax.optimization_barrier(([r.prepare() for r in reductions], inputs))
    for r, send in zip(reductions, sends):
        r.launch(send)
    return inputs if len(inputs) != 1 else inputs[0]


def matmul_tn(lhs, rhs):
    return jnp.einsum("bsf,bsd->fd", lhs, rhs, preferred_element_type=F32)


def column_halves(value, core):
    lead = value.shape[:2]
    parts = value.reshape(*lead, 2, 2, value.shape[2] // 4)
    return [pick(parts, idx, 3).reshape(*lead, -1) for idx in (core, 1 - core)]


def solution(mesh):
    fsdp_size = mesh.shape["fsdp"]
    batch_spec = P(("dp", "fsdp"), None, None)
    scale_spec = P(None, "fsdp")
    weight_spec = P(None, "fsdp", None)

    def device_step(x_in, grad_y, norm_scale, w_in, w_out):
        shard_rows = w_in.shape[1]
        seq_len, model_dim = x_in.shape[1:]
        ff_dim = w_out.shape[1] * fsdp_size - model_dim
        kv_end = model_dim + 128
        dims = (model_dim, ff_dim, seq_len, 768, 256)
        core = my_bit("core")
        tables = [jnp.asarray(t) for t in rotary_tables(seq_len, 64)]

        def gather(value):
            return lax.all_gather(value, "fsdp", axis=0, tiled=True)

        def project_out(hidden, mixed, weight):
            block_out = jnp.einsum("bsf,fd->bsd", mixed, weight, preferred_element_type=F32)
            return (hidden.astype(F32) + block_out).astype(BF16)

        gains = lax.all_gather(norm_scale, "fsdp", axis=1, tiled=True).astype(F32)
        gain0, gain1 = gains[0][None], gains[1][None]
        w_in0 = gather(w_in[0])
        w_out0 = gather(w_out[0])
        w_in1 = gather(w_in[1])
        w_out1 = gather(w_out[1])
        normed0, z0, gu0, mixed0 = layer_forward(x_in, gain0, w_in0, tables, dims)
        hidden1 = project_out(x_in, mixed0, w_out0)
        normed1, z1, gu1, mixed1 = layer_forward(hidden1, gain1, w_in1, tables, dims)

        out1 = Reduction(matmul_tn(mixed1, grad_y))
        keep1, give1 = column_halves(normed1, core)
        gu1, grad_y = advance([out1], gu1, grad_y)
        dgu1 = mlp_backward(grad_y, gu1, w_out1, dims)
        give1, dgu1 = advance([out1], give1, dgu1)
        up1 = Reduction(None, matmul_tn(give1, dgu1), relay="z")
        keep1, dgu1 = advance([up1], keep1, dgu1)
        up1.part = matmul_tn(keep1, dgu1)
        up1.part, z1, grad_y = advance([out1, up1], up1.part, z1, grad_y)
        dz1 = attention_backward(grad_y, z1, w_out1, tables, dims)
        dz1, dgu1, grad_y = advance([out1, up1], dz1, dgu1, grad_y)
        grad_h, scale1 = input_backward(grad_y, hidden1, gain1, dz1, dgu1, w_in1, dims)
        grad_h, mixed0, dz1 = advance([out1, up1], grad_h, mixed0, dz1)
        part_qkv1 = matmul_tn(normed1, dz1)
        out0 = Reduction(matmul_tn(mixed0, grad_h))

        keep0, give0 = column_halves(normed0, core)
        gu0, grad_h = advance([out1, up1, out0], gu0, grad_h)
        dgu0 = mlp_backward(grad_h, gu0, w_out0, dims)
        give0, dgu0 = advance([up1, out0], give0, dgu0)
        up0 = Reduction(None, matmul_tn(give0, dgu0), relay="z")
        keep0, dgu0 = advance([up0], keep0, dgu0)
        up0.part = matmul_tn(keep0, dgu0)
        up0.part, z0, grad_h = advance([out0, up0], up0.part, z0, grad_h)
        dz0 = attention_backward(grad_h, z0, w_out0, tables, dims)
        dz0, normed0 = advance([out0, up0], dz0, normed0)
        qkv = Reduction(jnp.concatenate([matmul_tn(normed0, dz0), part_qkv1], axis=1))
        dz0, dgu0, grad_h = advance([qkv], dz0, dgu0, grad_h)
        grad_x, scale0 = input_backward(grad_h, x_in, gain0, dz0, dgu0, w_in0, dims)
        scales = SmallSum(jnp.concatenate([scale0, scale1], axis=0))
        mixed1, grad_x = advance([out0, up0, qkv, scales], mixed1, grad_x)
        y_out = project_out(hidden1, mixed1, w_out1)
        y_out = advance([out0, up0, qkv, scales], y_out)
        y_out = advance([up0, qkv, scales], y_out)
        y_out = advance([qkv, scales], y_out)
        y_out = advance([qkv], y_out)
        grad_scale = lax.dynamic_slice_in_dim(scales.value, lax.axis_index("fsdp") * shard_rows, shard_rows, axis=1)

        out_in = jnp.zeros((2, shard_rows, w_in.shape[2]), F32)
        out_out = jnp.zeros((2, w_out.shape[1], model_dim), F32)
        for layer_idx, (wide, rows) in enumerate(((up0, out0), (up1, out1))):
            out_in = wide.place(out_in, layer_idx, kv_end)
            out_in = qkv.place(out_in, layer_idx, 0, layer_idx * kv_end, kv_end)
            out_out = rows.place(out_out, layer_idx, 0)
        return y_out, grad_x, grad_scale, out_in, out_out

    return jax.shard_map(
        device_step,
        mesh=mesh,
        in_specs=(batch_spec, batch_spec, scale_spec, weight_spec, weight_spec),
        out_specs=(batch_spec, batch_spec, scale_spec, weight_spec, weight_spec),
        check_vma=False,
    )
```

```python
import functools
import jax
import jax.numpy as jnp
import numpy as np
from jax import lax
from jax.experimental import pallas as pl
from jax.experimental.pallas import tpu as pltpu
from jax.sharding import PartitionSpec as P

F32 = jnp.float32
BF16 = jnp.bfloat16
VMEM_LIMIT = 67_043_328


def dot_nn(lhs, rhs):
    return lax.dot_general(lhs, rhs, (((1,), (0,)), ((), ())), preferred_element_type=F32)


def dot_nt(lhs, rhs):
    return lax.dot_general(lhs, rhs, (((1,), (1,)), ((), ())), preferred_element_type=F32)


def dot_tn(lhs, rhs):
    return lax.dot_general(lhs, rhs, (((0,), (0,)), ((), ())), preferred_element_type=F32)


def rotary_tables(seq_len, head_dim):
    half_dim = head_dim // 2
    inv_freq = 10000.0 ** (-(np.arange(half_dim, dtype=np.float64) * 2.0 / head_dim))
    angles = np.arange(seq_len, dtype=np.float64)[:, None] * inv_freq[None, :]
    cos_tab = np.tile(np.cos(angles), (1, 128 // half_dim))
    sin_tab = np.tile(np.concatenate([-np.sin(angles), np.sin(angles)], axis=1), (1, 128 // head_dim))
    return cos_tab.astype(np.float32), sin_tab.astype(np.float32)


def swap_halves(block):
    lane = lax.broadcasted_iota(jnp.int32, block.shape, 1)
    return jnp.where((lane & 63) < 32, pltpu.roll(block, 96, 1), pltpu.roll(block, 32, 1))


def lower_lanes(shape):
    return lax.broadcasted_iota(jnp.int32, shape, 1) < 64


def normalize(hidden):
    centered = hidden - jnp.mean(hidden, axis=-1, keepdims=True)
    variance = jnp.mean(centered * centered, axis=-1, keepdims=True)
    rstd = lax.rsqrt(variance + 1e-6)
    return centered * rstd, rstd


def causal_mask(scores, start, query_dim):
    size = scores.shape[1 - query_dim] - start
    square = scores[:, start:] if query_dim == 0 else scores[start:]
    query = lax.broadcasted_iota(jnp.int32, square.shape, query_dim) & (size - 1)
    square = jnp.where(query >= lax.broadcasted_iota(jnp.int32, square.shape, 1 - query_dim), square, -1e30)
    if start == 0:
        return square
    rest = scores[:, :start] if query_dim == 0 else scores[:start]
    return jnp.concatenate([rest, square], axis=1 - query_dim)


def attention_forward_kernel(x_ref, g_ref, w_ref, cos_ref, sin_ref, h_ref, z_ref, o_ref, k_lo, k_hi, v_lo, v_hi, *, dims):
    model_dim, ff_dim, seq_len, chunk, q_block = dims
    h = (normalize(x_ref[0].astype(F32))[0] * g_ref[...]).astype(BF16)
    h_ref[0] = h
    z_ref[0] = dot_nn(h, w_ref[...]).astype(BF16)

    kv = z_ref[0, :, model_dim:].astype(F32)
    low = lower_lanes(kv.shape)
    k_rot = jnp.where(low, kv * cos_ref[...] + swap_halves(kv) * sin_ref[...], 0.0)
    k_lo[...] = k_rot.astype(BF16)
    k_hi[...] = pltpu.roll(k_rot, 64, 1).astype(BF16)
    val = jnp.where(low, 0.0, kv)
    v_hi[...] = val.astype(BF16)
    v_lo[...] = pltpu.roll(val, 64, 1).astype(BF16)

    def head_pair(pair, carry):
        cols = pl.ds(pl.multiple_of(pair * 128, 128), 128)
        q = z_ref[0, :, cols].astype(F32) * 0.125
        q = (q * cos_ref[...] + swap_halves(q) * sin_ref[...]).astype(BF16)
        for blk in range(seq_len // q_block):
            start, n_keys = blk * q_block, (blk + 1) * q_block
            q_blk = q[start:n_keys]
            out = None
            for k_ref, v_ref in ((k_lo, v_lo), (k_hi, v_hi)):
                scores = causal_mask(dot_nt(q_blk, k_ref[:n_keys]), start, 0)
                probs = jnp.exp(scores - jnp.max(scores, axis=-1, keepdims=True))
                probs = probs * (1.0 / jnp.sum(probs, axis=-1, keepdims=True))
                part = dot_nn(probs.astype(BF16), v_ref[:n_keys])
                out = part if out is None else out + part
            o_ref[0, start:n_keys, cols] = out.astype(BF16)
        return carry

    lax.fori_loop(0, model_dim // 128, head_pair, 0)


def mlp_forward_kernel(h_ref, o_ref, w_ref, gu_ref, om_ref, *, dims):
    model_dim, ff_dim, seq_len, chunk, q_block = dims
    om_ref[0, :, :model_dim] = o_ref[0]

    def ff_chunk(idx, carry):
        base = pl.multiple_of(idx * chunk, 128)
        gate_cols = pl.ds(base, chunk)
        up_cols = pl.ds(pl.multiple_of(ff_dim + base, 128), chunk)
        gate = dot_nn(h_ref[0], w_ref[:, gate_cols]).astype(BF16)
        up = dot_nn(h_ref[0], w_ref[:, up_cols]).astype(BF16)
        gu_ref[0, :, gate_cols] = gate
        gu_ref[0, :, up_cols] = up
        gate = gate.astype(F32)
        mid = gate * jax.nn.sigmoid(gate) * up.astype(F32)
        om_ref[0, :, pl.ds(pl.multiple_of(model_dim + base, 128), chunk)] = mid.astype(BF16)
        return carry

    lax.fori_loop(0, ff_dim // chunk, ff_chunk, 0)


def mlp_backward_kernel(dy_ref, gu_ref, wout_ref, dgu_ref, *, dims):
    model_dim, ff_dim, seq_len, chunk, q_block = dims

    def ff_chunk(idx, carry):
        base = pl.multiple_of(idx * chunk, 128)
        gate_cols = pl.ds(base, chunk)
        up_cols = pl.ds(pl.multiple_of(ff_dim + base, 128), chunk)
        d_mid = dot_nt(dy_ref[0], wout_ref[pl.ds(pl.multiple_of(model_dim + base, 128), chunk), :]).astype(BF16).astype(F32)
        gate = gu_ref[0, :, gate_cols].astype(F32)
        up = gu_ref[0, :, up_cols].astype(F32)
        sig = jax.nn.sigmoid(gate)
        act = gate * sig
        dgu_ref[0, :, up_cols] = (d_mid * act).astype(BF16)
        dgu_ref[0, :, gate_cols] = (d_mid * up * (sig + act * (1.0 - sig))).astype(BF16)
        return carry

    lax.fori_loop(0, ff_dim // chunk, ff_chunk, 0)


def attention_backward_kernel(dy_ref, z_ref, wout_ref, cos_ref, sin_ref, *refs, dims):
    dz_ref, do_ref, k_lo, k_hi, k_dup, v_dup, dk_acc, dv_acc = refs[-8:]
    model_dim, ff_dim, seq_len, chunk, q_block = dims
    kv_end = model_dim + 128
    do_ref[...] = dot_nt(dy_ref[0], wout_ref[...]).astype(BF16)
    kv = z_ref[0, :, model_dim:kv_end].astype(F32)
    low = lower_lanes(kv.shape)
    k_rot = jnp.where(low, kv * cos_ref[...] + swap_halves(kv) * sin_ref[...], 0.0)
    k_up = pltpu.roll(k_rot, 64, 1)
    k_lo[...] = k_rot.astype(BF16)
    k_hi[...] = k_up.astype(BF16)
    k_dup[...] = (k_rot + k_up).astype(BF16)
    v_dup[...] = jnp.where(low, pltpu.roll(kv, 64, 1), kv).astype(BF16)
    dk_acc[...] = jnp.zeros_like(dk_acc)
    dv_acc[...] = jnp.zeros_like(dv_acc)

    def head_pair(pair, carry):
        cols = pl.ds(pl.multiple_of(pair * 128, 128), 128)
        q = z_ref[0, :, cols].astype(F32) * 0.125
        q = q * cos_ref[...] + swap_halves(q) * sin_ref[...]
        d_out = do_ref[:, cols].astype(F32)
        for blk in range(seq_len // q_block):
            start, n_keys = blk * q_block, (blk + 1) * q_block
            low_q = lower_lanes((q_block, 128))
            q_blk = q[start:n_keys]
            do_blk = d_out[start:n_keys]
            q_two = jnp.concatenate([jnp.where(low_q, q_blk, 0.0), jnp.where(low_q, 0.0, q_blk)], axis=0).astype(BF16)
            do_two = jnp.concatenate([jnp.where(low_q, do_blk, 0.0), jnp.where(low_q, 0.0, do_blk)], axis=0).astype(BF16)
            scores = causal_mask(dot_nt(k_dup[:n_keys], q_two), start, 1)
            probs = jnp.exp(scores - jnp.max(scores, axis=0, keepdims=True))
            probs = probs * (1.0 / jnp.sum(probs, axis=0, keepdims=True))
            d_probs = dot_nt(v_dup[:n_keys], do_two).astype(BF16).astype(F32)
            d_scores = (probs * (d_probs - jnp.sum(probs * d_probs, axis=0, keepdims=True))).astype(BF16)
            dv_acc[:n_keys] += dot_nn(probs.astype(BF16), do_two)
            dk_acc[:n_keys] += dot_nn(d_scores, q_two)
            dq = dot_tn(d_scores[:, :q_block], k_lo[:n_keys]) + dot_tn(d_scores[:, q_block:], k_hi[:n_keys])
            dq = dq.astype(BF16).astype(F32)
            dq = dq * cos_ref[start:n_keys] - swap_halves(dq) * sin_ref[start:n_keys]
            dz_ref[0, start:n_keys, cols] = (dq * 0.125).astype(BF16)
        return carry

    lax.fori_loop(0, model_dim // 128, head_pair, 0)
    dk = dk_acc[...]
    dk = (dk + pltpu.roll(dk, 64, 1)).astype(BF16).astype(F32)
    dk = dk * cos_ref[...] - swap_halves(dk) * sin_ref[...]
    dv = dv_acc[...]
    dv = dv + pltpu.roll(dv, 64, 1)
    dz_ref[0, :, model_dim:kv_end] = jnp.where(low, dk, dv).astype(BF16)


def input_backward_kernel(dy_ref, x_ref, g_ref, dz_ref, dgu_ref, wqkv_ref, wgu_ref, *refs, dims):
    model_dim = dims[0]
    dx_ref, dg_ref, dh_ref = refs[-3:]
    for start in range(0, model_dim, 256):
        rows = slice(start, start + 256)
        dh = dot_nt(dgu_ref[0], wgu_ref[rows, :]) + dot_nt(dz_ref[0], wqkv_ref[rows, :])
        dh_ref[:, rows] = dh.astype(BF16)
    x_hat, rstd = normalize(x_ref[0].astype(F32))
    dh = dh_ref[...].astype(F32)
    d_gain = jnp.sum(dh * x_hat, axis=0, keepdims=True)

    @pl.when(pl.program_id(0) == 0)
    def _():
        dg_ref[...] = d_gain

    @pl.when(pl.program_id(0) > 0)
    def _():
        dg_ref[...] += d_gain

    d_hat = dh * g_ref[...]
    d_in = rstd * (d_hat - jnp.mean(d_hat, axis=-1, keepdims=True)
                   - x_hat * jnp.mean(d_hat * x_hat, axis=-1, keepdims=True))
    dx_ref[0] = (dy_ref[0].astype(F32) + d_in.astype(BF16).astype(F32)).astype(BF16)


WHOLE = pl.BlockSpec(memory_space=pltpu.VMEM)


def seq_call(kernel, name, n_seq, inputs, seq_outputs, whole_outputs, scratch, flops, seq_len, span=None, into=None):
    first, count = span or (0, n_seq)

    def seq_spec(width):
        return pl.BlockSpec((1, seq_len, width), lambda i: (i + first, 0, 0) if first else (i, 0, 0))

    specs, arrays = [], []
    for value in inputs:
        if isinstance(value, tuple):
            value, rows = value
            specs.append(pl.BlockSpec((rows, value.shape[1]), lambda i: (0, 0)))
        else:
            specs.append(seq_spec(value.shape[2]) if value.ndim == 3 else WHOLE)
        arrays.append(value)
    aliases = {}
    if into is not None:
        aliases = {len(arrays): 0}
        specs.append(pl.BlockSpec(memory_space=pl.ANY))
        arrays.append(into)
    shapes = [jax.ShapeDtypeStruct((n_seq, seq_len, w), BF16) for w in seq_outputs]
    shapes += [jax.ShapeDtypeStruct(w, F32) for w in whole_outputs]
    return pl.pallas_call(
        kernel,
        grid=(count,),
        out_shape=shapes,
        in_specs=specs,
        out_specs=[seq_spec(w) for w in seq_outputs] + [pl.BlockSpec(w, lambda i: (0, 0)) for w in whole_outputs],
        scratch_shapes=scratch,
        input_output_aliases=aliases,
        compiler_params=pltpu.CompilerParams(dimension_semantics=("arbitrary",), vmem_limit_bytes=VMEM_LIMIT),
        cost_estimate=pl.CostEstimate(flops=flops * count // n_seq, bytes_accessed=50_000_000 * count // n_seq,
                                      transcendentals=0),
        name=name,
    )(*arrays)


def attention_forward(x, gain, w_qkv, tables, dims):
    model_dim, ff_dim, seq_len = dims[:3]
    return seq_call(functools.partial(attention_forward_kernel, dims=dims), "attention_forward", x.shape[0],
                    [x, gain, w_qkv, *tables], [model_dim, w_qkv.shape[1], model_dim], [],
                    [pltpu.VMEM((seq_len, 128), BF16)] * 4,
                    2 * x.shape[0] * seq_len * model_dim * (w_qkv.shape[1] + 4 * seq_len), seq_len)


def mlp_forward(h, o, w_gu, dims):
    model_dim, ff_dim, seq_len = dims[:3]
    return seq_call(functools.partial(mlp_forward_kernel, dims=dims), "mlp_forward", h.shape[0],
                    [h, o, w_gu], [2 * ff_dim, model_dim + ff_dim], [], [],
                    2 * h.shape[0] * seq_len * model_dim * 2 * ff_dim, seq_len)


def mlp_backward(dy, gu, w_out, dims):
    model_dim, ff_dim, seq_len = dims[:3]
    return seq_call(functools.partial(mlp_backward_kernel, dims=dims), "mlp_backward", dy.shape[0],
                    [dy, gu, w_out], [2 * ff_dim], [], [],
                    2 * dy.shape[0] * seq_len * model_dim * ff_dim, seq_len)[0]


def attention_backward(dy, z, w_out, tables, dims, span, into=None):
    model_dim, ff_dim, seq_len = dims[:3]
    small = pltpu.VMEM((seq_len, 128), BF16)
    wide = pltpu.VMEM((seq_len, 128), F32)
    return seq_call(functools.partial(attention_backward_kernel, dims=dims), "attention_backward", dy.shape[0],
                    [dy, z, (w_out, model_dim), *tables], [model_dim + 128], [],
                    [pltpu.VMEM((seq_len, model_dim), BF16), small, small, small, small, wide, wide],
                    2 * dy.shape[0] * seq_len * model_dim * (model_dim + 10 * seq_len), seq_len, span, into)[0]


def input_backward(dy, x, gain, dz, dgu, w_qkv, w_gu, dims, span, into=None):
    model_dim, ff_dim, seq_len = dims[:3]
    return seq_call(functools.partial(input_backward_kernel, dims=dims), "input_backward", dy.shape[0],
                    [dy, x, gain, dz, dgu, w_qkv, w_gu], [model_dim], [(1, model_dim)],
                    [pltpu.VMEM((seq_len, model_dim), BF16)],
                    2 * dy.shape[0] * seq_len * model_dim * (w_qkv.shape[1] + w_gu.shape[1]), seq_len, span, into)


LINKS = {"core": ("fsdp", 1), "x": ("fsdp", 2), "y": ("dp", 1), "z": ("dp", 2)}


def swap(value, link):
    axis, bit = LINKS[link]
    return lax.ppermute(value, axis, [(i, i ^ bit) for i in range(4)])


def my_bit(link):
    axis, bit = LINKS[link]
    return (lax.axis_index(axis) // bit) % 2


def pick(value, index, dim):
    return lax.dynamic_index_in_dim(value, index, dim, keepdims=False)


ORDERS = (("x", "y", "z"), ("y", "z", "x"), ("z", "x", "y"))
DIMS = ("x", "core", "y", "z")


class Reduction:
    def __init__(self, part, sent=None, relay="y"):
        core = my_bit("core")
        self.stage, self.relay = 0, relay
        self.cols = (part if sent is None else sent).shape[1]
        if sent is None:
            self.part = self.view(part, 2)
            self.sent = self.cut(self.part, {"core": 1 - core})
        else:
            self.part, self.sent = part, self.view(sent, 1)
        self.picks = [{"core": core} for _ in range(3)]
        self.terms = [[], [], []]

    def view(self, value, cores):
        rows = value.shape[0] // (2 * cores * 12)
        return value.reshape(2, cores, 2, 2, 3, rows, self.cols)

    def cut(self, term, picks, third=None):
        starts, sizes = [], []
        for dim, size in zip(DIMS, term.shape):
            starts.append(picks[dim] if dim in picks and size == 2 else 0)
            sizes.append(1 if dim in picks else size)
        whole = third is None or term.shape[4] == 1
        starts += [0 if whole else third, 0, 0]
        sizes += [term.shape[4] if whole else 1, *term.shape[5:]]
        return lax.dynamic_slice(term, starts, sizes)

    def total(self, third, picks):
        return sum(self.cut(t, picks, third) for t in self.terms[third])

    def prepare(self):
        if self.stage == 0:
            return [self.sent]
        if self.stage == 1:
            part = self.part if self.part.ndim == 7 else self.view(self.part, 1)
            self.terms = [[part, self.received[0]] for _ in range(3)]
        elif self.stage <= 4:
            for terms, received in zip(self.terms, self.received):
                terms.append(received)
        if self.stage <= 3:
            sends = []
            for third, order in enumerate(ORDERS):
                link = order[self.stage - 1]
                bit = my_bit(link)
                sends.append(self.total(third, {**self.picks[third], link: 1 - bit}))
                self.picks[third][link] = bit
            return sends
        if self.stage == 4:
            return [jnp.concatenate([self.total(third, self.picks[third]) for third in range(3)], axis=4)]
        return self.received if self.stage == 5 else [self.last]

    def launch(self, sends):
        if self.stage == 0:
            self.received = [swap(sends[0], "core")]
        elif self.stage <= 3:
            self.received = [swap(s, order[self.stage - 1]) for s, order in zip(sends, ORDERS)]
        elif self.stage == 4:
            self.own = sends[0]
            self.received = [swap(self.own, "y"), swap(self.own, "z")]
        elif self.stage == 5:
            self.received = sends
            self.last = swap(sends[0 if self.relay == "z" else 1], self.relay)
        else:
            self.last = sends[0]
        self.stage += 1

    def place(self, out, layer_idx, col, start=0, width=None):
        for piece, flip_y, flip_z in ((self.own, 0, 0), (self.received[0], 1, 0), (self.received[1], 0, 1), (self.last, 1, 1)):
            block = piece.reshape(1, -1, self.cols)[:, :, start:start + (width or self.cols)]
            row = (((my_bit("y") + flip_y) % 2) * 2 + (my_bit("z") + flip_z) % 2) * block.shape[1]
            out = lax.dynamic_update_slice(out, block, (layer_idx, row, col))
        return out


class SmallSum:
    def __init__(self, value):
        self.value, self.links = value, ["core", "x", "y", "z"]

    def prepare(self):
        return [self.value]

    def launch(self, sends):
        self.value = sends[0] + swap(sends[0], self.links.pop(0))


def advance(reductions, *inputs):
    sends, inputs = lax.optimization_barrier(([r.prepare() for r in reductions], inputs))
    for r, send in zip(reductions, sends):
        r.launch(send)
    return inputs if len(inputs) != 1 else inputs[0]


def matmul_tn(lhs, rhs):
    return jnp.einsum("bsf,bsd->fd", lhs, rhs, preferred_element_type=F32)


def column_halves(value, core):
    lead = value.shape[:2]
    parts = value.reshape(*lead, 2, 2, value.shape[2] // 4)
    return [pick(parts, idx, 3).reshape(*lead, -1) for idx in (core, 1 - core)]


def solution(mesh):
    fsdp_size = mesh.shape["fsdp"]
    batch_spec = P(("dp", "fsdp"), None, None)
    scale_spec = P(None, "fsdp")
    weight_spec = P(None, "fsdp", None)

    def device_step(x_in, grad_y, norm_scale, w_in, w_out):
        shard_rows = w_in.shape[1]
        seq_len, model_dim = x_in.shape[1:]
        ff_dim = w_out.shape[1] * fsdp_size - model_dim
        kv_end = model_dim + 128
        dims = (model_dim, ff_dim, seq_len, 768, 256)
        core = my_bit("core")
        tables = [jnp.asarray(t) for t in rotary_tables(seq_len, 64)]

        def gather(value):
            return lax.all_gather(value, "fsdp", axis=0, tiled=True)

        def project_out(hidden, mixed, weight):
            block_out = jnp.einsum("bsf,fd->bsd", mixed, weight, preferred_element_type=F32)
            return (hidden.astype(F32) + block_out).astype(BF16)

        half = x_in.shape[0] // 2
        low, high, every = (0, half), (half, x_in.shape[0] - half), (0, x_in.shape[0])

        gains = lax.all_gather(norm_scale, "fsdp", axis=1, tiled=True).astype(F32)
        gain0, gain1 = gains[0][None], gains[1][None]
        w_qkv0 = gather(w_in[0, :, :kv_end])
        w_gu0 = gather(w_in[0, :, kv_end:])
        w_out0 = gather(w_out[0])
        w_qkv1 = gather(w_in[1, :, :kv_end])
        w_gu1 = gather(w_in[1, :, kv_end:])
        w_out1 = gather(w_out[1])
        normed0, z0, heads0 = attention_forward(x_in, gain0, w_qkv0, tables, dims)
        gu0, mixed0 = mlp_forward(normed0, heads0, w_gu0, dims)
        hidden1 = project_out(x_in, mixed0, w_out0)
        normed1, z1, heads1 = attention_forward(hidden1, gain1, w_qkv1, tables, dims)
        gu1, mixed1 = mlp_forward(normed1, heads1, w_gu1, dims)

        out1 = Reduction(matmul_tn(mixed1, grad_y))
        keep1, give1 = column_halves(normed1, core)
        gu1, grad_y = advance([out1], gu1, grad_y)
        dgu1 = mlp_backward(grad_y, gu1, w_out1, dims)
        give1, dgu1 = advance([out1], give1, dgu1)
        up1 = Reduction(None, matmul_tn(give1, dgu1), relay="z")
        keep1, dgu1 = advance([up1], keep1, dgu1)
        up1.part = matmul_tn(keep1, dgu1)
        up1.part, z1, grad_y = advance([out1, up1], up1.part, z1, grad_y)
        dz1 = attention_backward(grad_y, z1, w_out1, tables, dims, low)
        dz1, z1, grad_y = advance([out1], dz1, z1, grad_y)
        dz1 = attention_backward(grad_y, z1, w_out1, tables, dims, high, dz1)
        dz1, dgu1, grad_y = advance([out1, up1], dz1, dgu1, grad_y)
        grad_h, scale1 = input_backward(grad_y, hidden1, gain1, dz1, dgu1, w_qkv1, w_gu1, dims, every)
        grad_h, mixed0, dz1 = advance([out1, up1], grad_h, mixed0, dz1)
        part_qkv1 = matmul_tn(normed1, dz1)
        out0 = Reduction(matmul_tn(mixed0, grad_h))

        keep0, give0 = column_halves(normed0, core)
        gu0, grad_h = advance([out1, up1, out0], gu0, grad_h)
        dgu0 = mlp_backward(grad_h, gu0, w_out0, dims)
        give0, dgu0 = advance([out0], give0, dgu0)
        up0 = Reduction(None, matmul_tn(give0, dgu0), relay="z")
        keep0, dgu0 = advance([up1, up0], keep0, dgu0)
        up0.part = matmul_tn(keep0, dgu0)
        up0.part, z0, grad_h = advance([out0, up0], up0.part, z0, grad_h)
        dz0 = attention_backward(grad_h, z0, w_out0, tables, dims, low)
        dz0, z0, grad_h = advance([out0, up1], dz0, z0, grad_h)
        dz0 = attention_backward(grad_h, z0, w_out0, tables, dims, high, dz0)
        dz0, normed0 = advance([out0, up0], dz0, normed0)
        qkv = Reduction(jnp.concatenate([matmul_tn(normed0, dz0), part_qkv1], axis=1))
        dz0, dgu0, grad_h = advance([qkv], dz0, dgu0, grad_h)
        grad_x, scale0 = input_backward(grad_h, x_in, gain0, dz0, dgu0, w_qkv0, w_gu0, dims, every)
        scales = SmallSum(jnp.concatenate([scale0, scale1], axis=0))
        mixed1, grad_x = advance([out0, up0, qkv, scales], mixed1, grad_x)
        y_out = project_out(hidden1, mixed1, w_out1)
        y_out = advance([up0, qkv, scales], y_out)
        y_out = advance([up0, qkv, scales], y_out)
        y_out = advance([qkv, scales], y_out)
        y_out = advance([qkv], y_out)
        grad_scale = lax.dynamic_slice_in_dim(scales.value, lax.axis_index("fsdp") * shard_rows, shard_rows, axis=1)

        out_in = jnp.zeros((2, shard_rows, w_in.shape[2]), F32)
        out_out = jnp.zeros((2, w_out.shape[1], model_dim), F32)
        for layer_idx, (wide, rows) in enumerate(((up0, out0), (up1, out1))):
            out_in = wide.place(out_in, layer_idx, kv_end)
            out_in = qkv.place(out_in, layer_idx, 0, layer_idx * kv_end, kv_end)
            out_out = rows.place(out_out, layer_idx, 0)
        return y_out, grad_x, grad_scale, out_in, out_out

    return jax.shard_map(
        device_step,
        mesh=mesh,
        in_specs=(batch_spec, batch_spec, scale_spec, weight_spec, weight_spec),
        out_specs=(batch_spec, batch_spec, scale_spec, weight_spec, weight_spec),
        check_vma=False,
    )
```

```python
import functools
import jax
import jax.numpy as jnp
import numpy as np
from jax import lax
from jax.experimental import pallas as pl
from jax.experimental.pallas import tpu as pltpu
from jax.sharding import PartitionSpec as P

F32 = jnp.float32
BF16 = jnp.bfloat16
VMEM_LIMIT = 67_043_328


def dot_nn(lhs, rhs):
    return lax.dot_general(lhs, rhs, (((1,), (0,)), ((), ())), preferred_element_type=F32)


def dot_nt(lhs, rhs):
    return lax.dot_general(lhs, rhs, (((1,), (1,)), ((), ())), preferred_element_type=F32)


def dot_tn(lhs, rhs):
    return lax.dot_general(lhs, rhs, (((0,), (0,)), ((), ())), preferred_element_type=F32)


def rotary_tables(seq_len, head_dim):
    half_dim = head_dim // 2
    inv_freq = 10000.0 ** (-(np.arange(half_dim, dtype=np.float64) * 2.0 / head_dim))
    angles = np.arange(seq_len, dtype=np.float64)[:, None] * inv_freq[None, :]
    cos_tab = np.tile(np.cos(angles), (1, 128 // half_dim))
    sin_tab = np.tile(np.concatenate([-np.sin(angles), np.sin(angles)], axis=1), (1, 128 // head_dim))
    return cos_tab.astype(np.float32), sin_tab.astype(np.float32)


def swap_halves(block):
    lane = lax.broadcasted_iota(jnp.int32, block.shape, 1)
    return jnp.where((lane & 63) < 32, pltpu.roll(block, 96, 1), pltpu.roll(block, 32, 1))


def lower_lanes(shape):
    return lax.broadcasted_iota(jnp.int32, shape, 1) < 64


def normalize(hidden):
    centered = hidden - jnp.mean(hidden, axis=-1, keepdims=True)
    variance = jnp.mean(centered * centered, axis=-1, keepdims=True)
    rstd = lax.rsqrt(variance + 1e-6)
    return centered * rstd, rstd


def causal_mask(scores, start, query_dim):
    size = scores.shape[1 - query_dim] - start
    square = scores[:, start:] if query_dim == 0 else scores[start:]
    query = lax.broadcasted_iota(jnp.int32, square.shape, query_dim) & (size - 1)
    square = jnp.where(query >= lax.broadcasted_iota(jnp.int32, square.shape, 1 - query_dim), square, -1e30)
    if start == 0:
        return square
    rest = scores[:, :start] if query_dim == 0 else scores[:start]
    return jnp.concatenate([rest, square], axis=1 - query_dim)


def attention_forward_kernel(x_ref, g_ref, w_ref, cos_ref, sin_ref, h_ref, z_ref, o_ref, h0_ref, h1_ref, k_lo, k_hi, v_lo, v_hi, *, dims):
    model_dim, ff_dim, seq_len, chunk, q_block = dims
    h = (normalize(x_ref[0].astype(F32))[0] * g_ref[...]).astype(BF16)
    h_ref[0] = h
    quarter = model_dim // 4
    quarters = [h[:, i * quarter:(i + 1) * quarter] for i in range(4)]
    h0_ref[0] = jnp.concatenate(quarters[0::2], axis=1)
    h1_ref[0] = jnp.concatenate(quarters[1::2], axis=1)
    z_ref[0] = dot_nn(h, w_ref[...]).astype(BF16)

    kv = z_ref[0, :, model_dim:].astype(F32)
    low = lower_lanes(kv.shape)
    k_rot = jnp.where(low, kv * cos_ref[...] + swap_halves(kv) * sin_ref[...], 0.0)
    k_lo[...] = k_rot.astype(BF16)
    k_hi[...] = pltpu.roll(k_rot, 64, 1).astype(BF16)
    val = jnp.where(low, 0.0, kv)
    v_hi[...] = val.astype(BF16)
    v_lo[...] = pltpu.roll(val, 64, 1).astype(BF16)

    def head_pair(pair, carry):
        cols = pl.ds(pl.multiple_of(pair * 128, 128), 128)
        q = z_ref[0, :, cols].astype(F32) * 0.125
        q = (q * cos_ref[...] + swap_halves(q) * sin_ref[...]).astype(BF16)
        for blk in range(seq_len // q_block):
            start, n_keys = blk * q_block, (blk + 1) * q_block
            q_blk = q[start:n_keys]
            out = None
            for k_ref, v_ref in ((k_lo, v_lo), (k_hi, v_hi)):
                scores = causal_mask(dot_nt(q_blk, k_ref[:n_keys]), start, 0)
                probs = jnp.exp(scores - jnp.max(scores, axis=-1, keepdims=True))
                probs = probs * (1.0 / jnp.sum(probs, axis=-1, keepdims=True))
                part = dot_nn(probs.astype(BF16), v_ref[:n_keys])
                out = part if out is None else out + part
            o_ref[0, start:n_keys, cols] = out.astype(BF16)
        return carry

    lax.fori_loop(0, model_dim // 128, head_pair, 0)


def mlp_forward_kernel(h_ref, o_ref, w_ref, gu_ref, om_ref, *, dims):
    model_dim, ff_dim, seq_len, chunk, q_block = dims
    om_ref[0, :, :model_dim] = o_ref[0]

    def ff_chunk(idx, carry):
        base = pl.multiple_of(idx * chunk, 128)
        gate_cols = pl.ds(base, chunk)
        up_cols = pl.ds(pl.multiple_of(ff_dim + base, 128), chunk)
        gate = dot_nn(h_ref[0], w_ref[:, gate_cols]).astype(BF16)
        up = dot_nn(h_ref[0], w_ref[:, up_cols]).astype(BF16)
        gu_ref[0, :, gate_cols] = gate
        gu_ref[0, :, up_cols] = up
        gate = gate.astype(F32)
        mid = gate * jax.nn.sigmoid(gate) * up.astype(F32)
        om_ref[0, :, pl.ds(pl.multiple_of(model_dim + base, 128), chunk)] = mid.astype(BF16)
        return carry

    lax.fori_loop(0, ff_dim // chunk, ff_chunk, 0)


def mlp_backward_kernel(dy_ref, gu_ref, wout_ref, dgu_ref, *, dims):
    model_dim, ff_dim, seq_len, chunk, q_block = dims

    def ff_chunk(idx, carry):
        base = pl.multiple_of(idx * chunk, 128)
        gate_cols = pl.ds(base, chunk)
        up_cols = pl.ds(pl.multiple_of(ff_dim + base, 128), chunk)
        d_mid = dot_nt(dy_ref[0], wout_ref[pl.ds(pl.multiple_of(model_dim + base, 128), chunk), :]).astype(BF16).astype(F32)
        gate = gu_ref[0, :, gate_cols].astype(F32)
        up = gu_ref[0, :, up_cols].astype(F32)
        sig = jax.nn.sigmoid(gate)
        act = gate * sig
        dgu_ref[0, :, up_cols] = (d_mid * act).astype(BF16)
        dgu_ref[0, :, gate_cols] = (d_mid * up * (sig + act * (1.0 - sig))).astype(BF16)
        return carry

    lax.fori_loop(0, ff_dim // chunk, ff_chunk, 0)


def attention_backward_kernel(dy_ref, z_ref, wout_ref, cos_ref, sin_ref, *refs, dims):
    dz_ref, do_ref, k_lo, k_hi, k_dup, v_dup, dk_acc, dv_acc = refs[-8:]
    model_dim, ff_dim, seq_len, chunk, q_block = dims
    kv_end = model_dim + 128
    do_ref[...] = dot_nt(dy_ref[0], wout_ref[...]).astype(BF16)
    kv = z_ref[0, :, model_dim:kv_end].astype(F32)
    low = lower_lanes(kv.shape)
    k_rot = jnp.where(low, kv * cos_ref[...] + swap_halves(kv) * sin_ref[...], 0.0)
    k_up = pltpu.roll(k_rot, 64, 1)
    k_lo[...] = k_rot.astype(BF16)
    k_hi[...] = k_up.astype(BF16)
    k_dup[...] = (k_rot + k_up).astype(BF16)
    v_dup[...] = jnp.where(low, pltpu.roll(kv, 64, 1), kv).astype(BF16)
    dk_acc[...] = jnp.zeros_like(dk_acc)
    dv_acc[...] = jnp.zeros_like(dv_acc)

    def head_pair(pair, carry):
        cols = pl.ds(pl.multiple_of(pair * 128, 128), 128)
        q = z_ref[0, :, cols].astype(F32) * 0.125
        q = q * cos_ref[...] + swap_halves(q) * sin_ref[...]
        d_out = do_ref[:, cols].astype(F32)
        for blk in range(seq_len // q_block):
            start, n_keys = blk * q_block, (blk + 1) * q_block
            low_q = lower_lanes((q_block, 128))
            q_blk = q[start:n_keys]
            do_blk = d_out[start:n_keys]
            q_two = jnp.concatenate([jnp.where(low_q, q_blk, 0.0), jnp.where(low_q, 0.0, q_blk)], axis=0).astype(BF16)
            do_two = jnp.concatenate([jnp.where(low_q, do_blk, 0.0), jnp.where(low_q, 0.0, do_blk)], axis=0).astype(BF16)
            scores = causal_mask(dot_nt(k_dup[:n_keys], q_two), start, 1)
            probs = jnp.exp(scores - jnp.max(scores, axis=0, keepdims=True))
            probs = probs * (1.0 / jnp.sum(probs, axis=0, keepdims=True))
            d_probs = dot_nt(v_dup[:n_keys], do_two).astype(BF16).astype(F32)
            d_scores = (probs * (d_probs - jnp.sum(probs * d_probs, axis=0, keepdims=True))).astype(BF16)
            dv_acc[:n_keys] += dot_nn(probs.astype(BF16), do_two)
            dk_acc[:n_keys] += dot_nn(d_scores, q_two)
            dq = dot_tn(d_scores[:, :q_block], k_lo[:n_keys]) + dot_tn(d_scores[:, q_block:], k_hi[:n_keys])
            dq = dq.astype(BF16).astype(F32)
            dq = dq * cos_ref[start:n_keys] - swap_halves(dq) * sin_ref[start:n_keys]
            dz_ref[0, start:n_keys, cols] = (dq * 0.125).astype(BF16)
        return carry

    lax.fori_loop(0, model_dim // 128, head_pair, 0)
    dk = dk_acc[...]
    dk = (dk + pltpu.roll(dk, 64, 1)).astype(BF16).astype(F32)
    dk = dk * cos_ref[...] - swap_halves(dk) * sin_ref[...]
    dv = dv_acc[...]
    dv = dv + pltpu.roll(dv, 64, 1)
    dz_ref[0, :, model_dim:kv_end] = jnp.where(low, dk, dv).astype(BF16)


def input_backward_kernel(dy_ref, x_ref, g_ref, dz_ref, dgu_ref, wqkv_ref, wgu_ref, *refs, dims):
    model_dim = dims[0]
    dx_ref, dg_ref, dh_ref = refs[-3:]
    for start in range(0, model_dim, 256):
        rows = slice(start, start + 256)
        dh = dot_nt(dgu_ref[0], wgu_ref[rows, :]) + dot_nt(dz_ref[0], wqkv_ref[rows, :])
        dh_ref[:, rows] = dh.astype(BF16)
    x_hat, rstd = normalize(x_ref[0].astype(F32))
    dh = dh_ref[...].astype(F32)
    d_gain = jnp.sum(dh * x_hat, axis=0, keepdims=True)

    @pl.when(pl.program_id(0) == 0)
    def _():
        dg_ref[...] = d_gain

    @pl.when(pl.program_id(0) > 0)
    def _():
        dg_ref[...] += d_gain

    d_hat = dh * g_ref[...]
    d_in = rstd * (d_hat - jnp.mean(d_hat, axis=-1, keepdims=True)
                   - x_hat * jnp.mean(d_hat * x_hat, axis=-1, keepdims=True))
    dx_ref[0] = (dy_ref[0].astype(F32) + d_in.astype(BF16).astype(F32)).astype(BF16)


WHOLE = pl.BlockSpec(memory_space=pltpu.VMEM)


def seq_call(kernel, name, n_seq, inputs, seq_outputs, whole_outputs, scratch, flops, seq_len, span=None, into=None):
    first, count = span or (0, n_seq)

    def seq_spec(width):
        return pl.BlockSpec((1, seq_len, width), lambda i: (i + first, 0, 0) if first else (i, 0, 0))

    specs, arrays = [], []
    for value in inputs:
        if isinstance(value, tuple):
            value, rows = value
            specs.append(pl.BlockSpec((rows, value.shape[1]), lambda i: (0, 0)))
        else:
            specs.append(seq_spec(value.shape[2]) if value.ndim == 3 else WHOLE)
        arrays.append(value)
    aliases = {}
    if into is not None:
        aliases = {len(arrays): 0}
        specs.append(pl.BlockSpec(memory_space=pl.ANY))
        arrays.append(into)
    shapes = [jax.ShapeDtypeStruct((n_seq, seq_len, w), BF16) for w in seq_outputs]
    shapes += [jax.ShapeDtypeStruct(w, F32) for w in whole_outputs]
    return pl.pallas_call(
        kernel,
        grid=(count,),
        out_shape=shapes,
        in_specs=specs,
        out_specs=[seq_spec(w) for w in seq_outputs] + [pl.BlockSpec(w, lambda i: (0, 0)) for w in whole_outputs],
        scratch_shapes=scratch,
        input_output_aliases=aliases,
        compiler_params=pltpu.CompilerParams(dimension_semantics=("arbitrary",), vmem_limit_bytes=VMEM_LIMIT),
        cost_estimate=pl.CostEstimate(flops=flops * count // n_seq, bytes_accessed=50_000_000 * count // n_seq,
                                      transcendentals=0),
        name=name,
    )(*arrays)


def attention_forward(x, gain, w_qkv, tables, dims):
    model_dim, ff_dim, seq_len = dims[:3]
    return seq_call(functools.partial(attention_forward_kernel, dims=dims), "attention_forward", x.shape[0],
                    [x, gain, w_qkv, *tables], [model_dim, w_qkv.shape[1], model_dim, model_dim // 2, model_dim // 2], [],
                    [pltpu.VMEM((seq_len, 128), BF16)] * 4,
                    2 * x.shape[0] * seq_len * model_dim * (w_qkv.shape[1] + 4 * seq_len), seq_len)


def mlp_forward(h, o, w_gu, dims):
    model_dim, ff_dim, seq_len = dims[:3]
    return seq_call(functools.partial(mlp_forward_kernel, dims=dims), "mlp_forward", h.shape[0],
                    [h, o, w_gu], [2 * ff_dim, model_dim + ff_dim], [], [],
                    2 * h.shape[0] * seq_len * model_dim * 2 * ff_dim, seq_len)


def mlp_backward(dy, gu, w_out, dims):
    model_dim, ff_dim, seq_len = dims[:3]
    return seq_call(functools.partial(mlp_backward_kernel, dims=dims), "mlp_backward", dy.shape[0],
                    [dy, gu, w_out], [2 * ff_dim], [], [],
                    2 * dy.shape[0] * seq_len * model_dim * ff_dim, seq_len)[0]


def attention_backward(dy, z, w_out, tables, dims, span, into=None):
    model_dim, ff_dim, seq_len = dims[:3]
    small = pltpu.VMEM((seq_len, 128), BF16)
    wide = pltpu.VMEM((seq_len, 128), F32)
    return seq_call(functools.partial(attention_backward_kernel, dims=dims), "attention_backward", dy.shape[0],
                    [dy, z, (w_out, model_dim), *tables], [model_dim + 128], [],
                    [pltpu.VMEM((seq_len, model_dim), BF16), small, small, small, small, wide, wide],
                    2 * dy.shape[0] * seq_len * model_dim * (model_dim + 10 * seq_len), seq_len, span, into)[0]


def input_backward(dy, x, gain, dz, dgu, w_qkv, w_gu, dims, span, into=None):
    model_dim, ff_dim, seq_len = dims[:3]
    return seq_call(functools.partial(input_backward_kernel, dims=dims), "input_backward", dy.shape[0],
                    [dy, x, gain, dz, dgu, w_qkv, w_gu], [model_dim], [(1, model_dim)],
                    [pltpu.VMEM((seq_len, model_dim), BF16)],
                    2 * dy.shape[0] * seq_len * model_dim * (w_qkv.shape[1] + w_gu.shape[1]), seq_len, span, into)


LINKS = {"core": ("fsdp", 1), "x": ("fsdp", 2), "y": ("dp", 1), "z": ("dp", 2)}


def swap(value, link):
    axis, bit = LINKS[link]
    return lax.ppermute(value, axis, [(i, i ^ bit) for i in range(4)])


def my_bit(link):
    axis, bit = LINKS[link]
    return (lax.axis_index(axis) // bit) % 2


def pick(value, index, dim):
    return lax.dynamic_index_in_dim(value, index, dim, keepdims=False)


ORDERS = (("x", "y", "z"), ("y", "z", "x"), ("z", "x", "y"))
DIMS = ("x", "core", "y", "z")


class Reduction:
    def __init__(self, part, sent=None, relay=0):
        core = my_bit("core")
        self.stage, self.relay = 0, relay
        self.cols = (part if sent is None else sent).shape[1]
        if sent is None:
            self.part = self.view(part, 2)
            self.sent = self.cut(self.part, {"core": 1 - core})
        else:
            self.part, self.sent = part, self.view(sent, 1)
        self.picks = [{"core": core} for _ in range(3)]
        self.terms = [[], [], []]

    def view(self, value, cores):
        rows = value.shape[0] // (2 * cores * 12)
        return value.reshape(2, cores, 2, 2, 3, rows, self.cols)

    def cut(self, term, picks, third=None):
        starts, sizes = [], []
        for dim, size in zip(DIMS, term.shape):
            starts.append(picks[dim] if dim in picks and size == 2 else 0)
            sizes.append(1 if dim in picks else size)
        whole = third is None or term.shape[4] == 1
        starts += [0 if whole else third, 0, 0]
        sizes += [term.shape[4] if whole else 1, *term.shape[5:]]
        return lax.dynamic_slice(term, starts, sizes)

    def total(self, third, picks):
        return sum(self.cut(t, picks, third) for t in self.terms[third])

    def prepare(self):
        if self.stage == 0:
            return [self.sent]
        if self.stage == 1:
            part = self.part if self.part.ndim == 7 else self.view(self.part, 1)
            self.terms = [[part, self.received[0]] for _ in range(3)]
        elif self.stage <= 4:
            for terms, received in zip(self.terms, self.received):
                terms.append(received)
        if self.stage <= 3:
            sends = []
            for third, order in enumerate(ORDERS):
                link = order[self.stage - 1]
                bit = my_bit(link)
                sends.append(self.total(third, {**self.picks[third], link: 1 - bit}))
                self.picks[third][link] = bit
            return sends
        if self.stage == 4:
            return [jnp.concatenate([self.total(third, self.picks[third]) for third in range(3)], axis=4)]
        if self.stage == 5:
            return self.received
        return self.last

    def launch(self, sends):
        if self.stage == 0:
            self.received = [swap(sends[0], "core")]
        elif self.stage <= 3:
            self.received = [swap(s, order[self.stage - 1]) for s, order in zip(sends, ORDERS)]
        elif self.stage == 4:
            self.own = sends[0]
            self.received = [swap(self.own, "y"), swap(self.own, "z")]
        elif self.stage == 5:
            self.received = sends
            self.last = []
            if self.relay > 0:
                self.last.append(swap(sends[0][:, :, :, :, :self.relay], "z"))
            if self.relay < 3:
                self.last.append(swap(sends[1][:, :, :, :, self.relay:], "y"))
        else:
            self.last = sends
        self.stage += 1

    def place(self, out, layer_idx, col, start=0, width=None):
        height = self.own.shape[4] * self.own.shape[5]
        blocks = [(self.own, 0, 0, 0), (self.received[0], 1, 0, 0), (self.received[1], 0, 1, 0)]
        offset = 0
        for piece in self.last:
            blocks.append((piece, 1, 1, offset))
            offset += piece.shape[4] * piece.shape[5]
        for piece, flip_y, flip_z, offset in blocks:
            block = piece.reshape(1, -1, self.cols)[:, :, start:start + (width or self.cols)]
            row = (((my_bit("y") + flip_y) % 2) * 2 + (my_bit("z") + flip_z) % 2) * height + offset
            out = lax.dynamic_update_slice(out, block, (layer_idx, row, col))
        return out


class SmallSum:
    def __init__(self, value):
        self.value, self.links = value, ["core", "x", "y", "z"]

    def prepare(self):
        return [self.value]

    def launch(self, sends):
        self.value = sends[0] + swap(sends[0], self.links.pop(0))


def advance(reductions, *inputs):
    sends, inputs = lax.optimization_barrier(([r.prepare() for r in reductions], inputs))
    for r, send in zip(reductions, sends):
        r.launch(send)
    return inputs if len(inputs) != 1 else inputs[0]


def matmul_tn(lhs, rhs):
    return jnp.einsum("bsf,bsd->fd", lhs, rhs, preferred_element_type=F32)


def by_core(first, second, core):
    return jnp.where(core == 0, first, second), jnp.where(core == 0, second, first)


def solution(mesh):
    fsdp_size = mesh.shape["fsdp"]
    batch_spec = P(("dp", "fsdp"), None, None)
    scale_spec = P(None, "fsdp")
    weight_spec = P(None, "fsdp", None)

    def device_step(x_in, grad_y, norm_scale, w_in, w_out):
        shard_rows = w_in.shape[1]
        seq_len, model_dim = x_in.shape[1:]
        ff_dim = w_out.shape[1] * fsdp_size - model_dim
        kv_end = model_dim + 128
        dims = (model_dim, ff_dim, seq_len, 1536, 256)
        core = my_bit("core")
        tables = [jnp.asarray(t) for t in rotary_tables(seq_len, 64)]

        def gather(value):
            return lax.all_gather(value, "fsdp", axis=0, tiled=True)

        def project_out(hidden, mixed, weight):
            block_out = jnp.einsum("bsf,fd->bsd", mixed, weight, preferred_element_type=F32)
            return (hidden.astype(F32) + block_out).astype(BF16)

        half = x_in.shape[0] // 2
        low, high, every = (0, half), (half, x_in.shape[0] - half), (0, x_in.shape[0])

        gains = lax.all_gather(norm_scale, "fsdp", axis=1, tiled=True).astype(F32)
        gain0, gain1 = gains[0][None], gains[1][None]
        w_qkv0 = gather(w_in[0, :, :kv_end])
        w_gu0 = gather(w_in[0, :, kv_end:])
        w_out0 = gather(w_out[0])
        w_qkv1 = gather(w_in[1, :, :kv_end])
        w_gu1 = gather(w_in[1, :, kv_end:])
        w_out1 = gather(w_out[1])
        normed0, z0, heads0, *halves0 = attention_forward(x_in, gain0, w_qkv0, tables, dims)
        gu0, mixed0 = mlp_forward(normed0, heads0, w_gu0, dims)
        hidden1 = project_out(x_in, mixed0, w_out0)
        normed1, z1, heads1, *halves1 = attention_forward(hidden1, gain1, w_qkv1, tables, dims)
        gu1, mixed1 = mlp_forward(normed1, heads1, w_gu1, dims)

        out1 = Reduction(matmul_tn(mixed1, grad_y))
        keep1, give1 = by_core(*halves1, core)
        gu1, grad_y = advance([out1], gu1, grad_y)
        dgu1 = mlp_backward(grad_y, gu1, w_out1, dims)
        give1, dgu1 = advance([out1], give1, dgu1)
        up1 = Reduction(None, matmul_tn(give1, dgu1), relay=3)
        keep1, dgu1 = advance([up1], keep1, dgu1)
        up1.part = matmul_tn(keep1, dgu1)
        up1.part, z1, grad_y = advance([out1, up1], up1.part, z1, grad_y)
        dz1 = attention_backward(grad_y, z1, w_out1, tables, dims, low)
        dz1, z1, grad_y = advance([out1], dz1, z1, grad_y)
        dz1 = attention_backward(grad_y, z1, w_out1, tables, dims, high, dz1)
        dz1, dgu1, grad_y = advance([out1, up1], dz1, dgu1, grad_y)
        grad_h, scale1 = input_backward(grad_y, hidden1, gain1, dz1, dgu1, w_qkv1, w_gu1, dims, every)
        grad_h, mixed0, dz1 = advance([out1, up1], grad_h, mixed0, dz1)
        part_qkv1 = matmul_tn(normed1, dz1)
        out0 = Reduction(matmul_tn(mixed0, grad_h))

        keep0, give0 = by_core(*halves0, core)
        gu0, grad_h = advance([out1, up1, out0], gu0, grad_h)
        dgu0 = mlp_backward(grad_h, gu0, w_out0, dims)
        give0, dgu0 = advance([out0], give0, dgu0)
        up0 = Reduction(None, matmul_tn(give0, dgu0), relay=1)
        keep0, dgu0 = advance([up1, up0], keep0, dgu0)
        up0.part = matmul_tn(keep0, dgu0)
        up0.part, z0, grad_h = advance([out0, up0], up0.part, z0, grad_h)
        dz0 = attention_backward(grad_h, z0, w_out0, tables, dims, low)
        dz0, z0, grad_h = advance([out0, up1], dz0, z0, grad_h)
        dz0 = attention_backward(grad_h, z0, w_out0, tables, dims, high, dz0)
        dz0, normed0 = advance([out0, up0], dz0, normed0)
        qkv = Reduction(jnp.concatenate([matmul_tn(normed0, dz0), part_qkv1], axis=1))
        dz0, dgu0, grad_h = advance([qkv], dz0, dgu0, grad_h)
        grad_x, scale0 = input_backward(grad_h, x_in, gain0, dz0, dgu0, w_qkv0, w_gu0, dims, every)
        scales = SmallSum(jnp.concatenate([scale0, scale1], axis=0))
        mixed1, grad_x = advance([out0, up0, qkv, scales], mixed1, grad_x)
        y_out = project_out(hidden1, mixed1, w_out1)
        y_out = advance([qkv, scales, up0], y_out)
        y_out = advance([qkv, scales], y_out)
        y_out = advance([qkv, scales], y_out)
        y_out = advance([qkv, up0], y_out)
        grad_scale = lax.dynamic_slice_in_dim(scales.value, lax.axis_index("fsdp") * shard_rows, shard_rows, axis=1)

        out_in = jnp.zeros((2, shard_rows, w_in.shape[2]), F32)
        out_out = jnp.zeros((2, w_out.shape[1], model_dim), F32)
        for layer_idx, (wide, rows) in enumerate(((up0, out0), (up1, out1))):
            out_in = wide.place(out_in, layer_idx, kv_end)
            out_in = qkv.place(out_in, layer_idx, 0, layer_idx * kv_end, kv_end)
            out_out = rows.place(out_out, layer_idx, 0)
        return y_out, grad_x, grad_scale, out_in, out_out

    return jax.shard_map(
        device_step,
        mesh=mesh,
        in_specs=(batch_spec, batch_spec, scale_spec, weight_spec, weight_spec),
        out_specs=(batch_spec, batch_spec, scale_spec, weight_spec, weight_spec),
        check_vma=False,
    )
```
